32 devices in a mesh: freq: 4 (over x, core), rec: 8 (over z, y).
Axes of the slice: x: 2, y: 2, z: 4, core: 2. Of those that a mesh axis runs over, the one named last changes fastest.
Arguments:
- response_real: float32 [96, 1536, 1536], P('freq', 'rec'), may hold values from -0.109375 to 0.109375
- response_imaginary: float32 [96, 1536, 1536], P('freq', 'rec'), may hold values from -0.109375 to 0.109375
- focus: float32 [1536, 96, 128], P('rec', 'freq'), may hold values from -6 to 6
- initial: float32 [1536, 96, 128], P('rec', 'freq'), may hold values from -6 to 6
- onset: int32 [1536, 64], P('rec'), may hold values from 24 to 167
Outputs:
- focus_next: float32 [1536, 96, 128], P('rec', 'freq')
The draws below stay inside these ranges and needn't reach their ends.
All inputs are finite; a program needn't handle non-finite values.
Results may differ from the reference program's by a relative error of at most 0.0003.
Values sent between devices are 32-bit elements; how exact they have to be, the bound alone decides.
A program may use at most 192 MiB of HBM per device.

```python
import math
import jax
import jax.numpy as jnp
from jax import lax

F = 96
NPOS = 1536
P_SIZE = 64
NT = 192


def set_ends(drawn, own_key, least, top_value):
    dims = drawn.shape
    place = [jax.random.randint(jax.random.fold_in(own_key, axis), (), 0, dims[axis]) for axis in range(len(dims))]
    drawn = drawn.at[tuple(place)].set(least)
    longest = dims.index(max(dims))
    place[longest] = (place[longest] + 1) % dims[longest]
    return drawn.at[tuple(place)].set(top_value)


def shard_levels(stream_key, shape, pieces, smallest, top_value):
    factor_of = 1.0
    for axis_at, blocks in pieces:
        steps = jax.random.uniform(jax.random.fold_in(jax.random.fold_in(stream_key, 6), axis_at), (blocks,), jnp.float32, smallest / len(pieces), top_value / len(pieces))
        factor_of = factor_of * jnp.repeat(jnp.exp(steps), shape[axis_at] // blocks).reshape((-1,) + (1,) * (len(shape) - 1 - axis_at))
    return factor_of


def scatter_about(stream_key, dims, spread, most, cuts=(), held_as=jnp.bfloat16):
    level = shard_levels(stream_key, dims, cuts, -0.22, 0.18) if cuts else 1.0
    values = jax.random.normal(stream_key, dims, jnp.float32) * spread * level
    return jnp.minimum(jnp.maximum(values, -most), most).astype(held_as)


def setup_inputs(seed: int = 0) -> dict:
    key_of = jax.random.split(jax.random.key(seed), 6)
    return {
        "response_real": scatter_about(key_of[0], (F, NPOS, NPOS), (2 * NPOS) ** -0.5, 0.109375, ((0, 4), (1, 8)), jnp.float32),
        "response_imaginary": scatter_about(key_of[1], (F, NPOS, NPOS), (2 * NPOS) ** -0.5, 0.109375, ((0, 4), (1, 8)), jnp.float32),
        "focus": scatter_about(key_of[2], (NPOS, F, 2 * P_SIZE), 1.0, 6.0, ((0, 8), (1, 4)), jnp.float32),
        "initial": scatter_about(key_of[3], (NPOS, F, 2 * P_SIZE), 1.0, 6.0, ((0, 8), (1, 4)), jnp.float32),
        "onset": set_ends(jax.random.randint(key_of[4], (NPOS, P_SIZE), NT // 8, NT - NT // 8), jax.random.fold_in(key_of[4], 1), NT // 8, (NT - NT // 8) - 1).astype(jnp.int32),
    }


def tables(freqs):
    samples = 2 * freqs
    order = lax.iota(jnp.int32, freqs)
    sample = lax.iota(jnp.int32, samples)
    phase = (order[:, None] * sample[None, :]) % samples
    phases = (2.0 * math.pi / samples) * phase.astype(jnp.float32)
    cosine = jnp.cos(phases)
    sine = jnp.sin(phases)
    factor = jnp.where(order == 0, 1.0, 2.0).astype(jnp.float32)[:, None] / samples
    inverse = jnp.stack([factor * cosine, -factor * sine])
    forward = jnp.stack([cosine, -sine])
    return inverse, forward, sample


def window(spectrum, onset):
    count, freqs, width = spectrum.shape
    half = width // 2
    inverse, forward, sample = tables(freqs)
    split = spectrum.reshape(count, freqs, 2, half)
    traces = jnp.einsum("nkcp,ckt->ntp", split, inverse, precision=lax.Precision.HIGHEST)
    keep = sample[None, :, None] < onset[:, None, :]
    clipped = jnp.where(keep, traces, 0.0)
    back = jnp.einsum("ntp,ckt->nkcp", clipped, forward, precision=lax.Precision.HIGHEST)
    return back.reshape(count, freqs, width)


def adjoint_terms(real_part, imag_part, values):
    half = values.shape[2] // 2
    first = jnp.einsum("frs,rfq->sfq", real_part, values, precision=lax.Precision.HIGHEST)
    second = jnp.einsum("frs,rfq->sfq", imag_part, values, precision=lax.Precision.HIGHEST)
    return jnp.concatenate([first[..., :half] + second[..., half:], first[..., half:] - second[..., :half]], axis=2)


def forward_terms(real_part, imag_part, values):
    half = values.shape[2] // 2
    first = jnp.einsum("frs,sfq->rfq", real_part, values, precision=lax.Precision.HIGHEST)
    second = jnp.einsum("frs,sfq->rfq", imag_part, values, precision=lax.Precision.HIGHEST)
    return jnp.concatenate([first[..., :half] - second[..., half:], first[..., half:] + second[..., :half]], axis=2)


def reference(response_real, response_imaginary, focus, initial, onset):
    adjoint = adjoint_terms(response_real, response_imaginary, focus)
    windowed = window(adjoint, onset)
    forward = forward_terms(response_real, response_imaginary, windowed)
    return initial - window(forward, onset)
```

```python
import functools
import math

import jax
import jax.numpy as jnp
import numpy as np
from jax import lax
from jax.experimental import pallas as pl
from jax.experimental.pallas import tpu as pltpu
from jax.sharding import PartitionSpec as P

CORES = 2
SUBS = 2
VMEM_LIMIT = 63 * 2**20
MESH = pl.DeviceIdType.MESH
ANY = pl.BlockSpec(memory_space=pl.ANY)
IN_VMEM = pl.BlockSpec(memory_space=pltpu.VMEM)


class Place:
    def __init__(self):
        total = lax.axis_size("rec")
        ys = 1 << ((total.bit_length() - 1) // 2)
        self.Y = ys if total % ys == 0 else 1
        self.Z = total // self.Y
        self.FQ = lax.axis_size("freq")
        self.X = self.FQ // CORES
        self.rec = lax.axis_index("rec")
        self.freq = lax.axis_index("freq")
        self.z, self.y = self.rec // self.Y, self.rec % self.Y
        self.x, self.c = self.freq // CORES, self.freq % CORES
        self.down_hops, self.up_hops = self.Z - 1 - self.z, self.z
        self.bottom, self.top = self.z == 0, self.z == self.Z - 1
        self.corner = jnp.logical_or(self.bottom, self.top)
        self.end = jnp.where(self.bottom, 0, 1)
        self.unit = self.end * self.Y + self.y

    def above(self):
        return (self.freq, self.rec + self.Y)

    def below(self):
        return (self.freq, self.rec - self.Y)

    def beside(self, dy):
        return (self.freq, self.z * self.Y + (self.y + dy) % self.Y)


def remote(src, dst, send, recv, device):
    return pltpu.make_async_remote_copy(src, dst, send, recv, device_id=device, device_id_type=MESH)


def within(k, count):
    return jnp.logical_and(k >= 0, k < count)


def both(a, b):
    return jnp.logical_and(a, b)


def split(x):
    high = x.astype(jnp.bfloat16)
    return high, (x - high.astype(jnp.float32)).astype(jnp.bfloat16)


def loop(count, body):
    lax.fori_loop(0, count, lambda k, _: (body(k), 0)[1], 0)


def fetch_response(real_ref, imag_ref, buf, sems, f):
    slots = buf.shape[0]
    rows = buf.shape[1] // 2
    slot = f % slots
    return [
        pltpu.make_async_copy(ref.at[f], buf.at[slot, pl.ds(k * rows, rows)], sems.at[slot, k])
        for k, ref in enumerate((real_ref, imag_ref))
    ]


def spread(p, f, half, src, dst, own_sem, send, recv):
    nf = dst.shape[0] // p.FQ
    row = p.freq * nf + f
    for dx in range(p.X):
        target = ((p.x + dx) % p.X * CORES + half, p.rec)
        copy = remote(src, dst.at[row], send.at[half, dx, f], recv.at[p.freq, f], target)
        if dx == 0:
            mine = p.c == half

            @pl.when(mine)
            def _():
                pltpu.make_async_copy(src, dst.at[row], own_sem.at[f]).start()

            @pl.when(jnp.logical_not(mine))
            def _():
                copy.start()
        else:
            copy.start()


def spread_wait(p, f, src, dst, own_sem, send, recv):
    nf = dst.shape[0] // p.FQ
    pltpu.make_async_copy(src, dst.at[p.freq * nf + f], own_sem.at[f]).wait()
    for half in range(CORES):
        for dx in range(p.X):
            copy = remote(src, dst.at[f], send.at[half, dx, f], recv.at[p.freq, f], (p.freq, p.rec))
            if dx == 0:

                @pl.when(p.c != half)
                def _():
                    copy.wait_send()
            else:
                copy.wait_send()
    for source in range(p.FQ):

        @pl.when(p.freq != source)
        def _():
            remote(src, dst.at[source * nf + f], send.at[0, 0, f], recv.at[source, f], (p.freq, p.rec)).wait_recv()


def adjoint_kernel(focus_ref, onset_ref, real_ref, imag_ref, out_ref, own_onset_ref, *scratch):
    (term, buf, ry, rd1, ru1, rd2, ru2, rf) = scratch[:8]
    (fetch_sem, sy, qy, sd1, qd1, su1, qu1, sd2, qd2, su2, qu2, sf, qf, own_sem, sx, qx, so, qo) = scratch[8:]
    p = Place()
    nf, _, Y, SU, width = term.shape
    slots = buf.shape[0]
    pairs = nf // 2
    count = pairs * SUBS
    SR, SH = SU // SUBS, SU // CORES
    H = p.Z // 2
    U = 2 * Y
    nr = buf.shape[1] // 2
    sign = jnp.where(lax.broadcasted_iota(jnp.int32, (1, width), 1) < width // 2, 1.0, -1.0)

    def fetch(f):
        return fetch_response(real_ref, imag_ref, buf, fetch_sem, f)

    for f in range(min(slots, nf)):
        for copy in fetch(f):
            copy.start()

    owner = p.rec // H
    owner_rec = owner // Y * (p.Z - 1) * Y + owner % Y
    onset_rows = onset_ref.shape[0]

    def onset_copy(at):
        dst = own_onset_ref.at[pl.ds(at * onset_rows, onset_rows)]
        return remote(onset_ref, dst, so.at[0], qo.at[at], (p.freq, owner_rec))

    @pl.when(owner_rec == p.rec)
    def _():
        at = p.rec % H
        pltpu.make_async_copy(onset_ref, own_onset_ref.at[pl.ds(at * onset_rows, onset_rows)], so.at[1]).start()

    @pl.when(owner_rec != p.rec)
    def _():
        onset_copy(p.rec % H).start()

    def compute(f):
        for copy in fetch(f):
            copy.wait()
        slot = f % slots
        x = focus_ref[pl.ds(f, nr, stride=nf), :]
        crossed = pltpu.roll(x, width // 2, 1) * sign
        z_high, z_low = split(jnp.concatenate([x, crossed], axis=0).T)
        z = jnp.concatenate([z_high, z_low], axis=0)
        for u in range(0, U, 2):
            high, low = split(buf[slot, :, u * SU : (u + 2) * SU])
            wide = jnp.dot(z, high, preferred_element_type=jnp.float32)
            rest = jnp.dot(z_high, low, preferred_element_type=jnp.float32)
            total = wide[:width] + wide[width:] + rest
            term[f, u // Y, u % Y : u % Y + 2] = total.T.reshape(2, SU, width)

        @pl.when(f + slots < nf)
        def _():
            for copy in fetch(f + slots):
                copy.start()

    def rows_of(k):
        return pl.ds(k % SUBS * SR, SR)

    def halves(k):
        return range(CORES) if SUBS == 1 else [k % SUBS]

    def deliver(f, k):
        if SUBS == 1:
            for half in range(CORES):
                spread(p, f, half, term.at[f, p.end, p.y, pl.ds(half * SH, SH)], out_ref, own_sem, sx, qx)
        else:
            for half in range(CORES):

                @pl.when(k % SUBS == half)
                def _():
                    spread(p, f, half, term.at[f, p.end, p.y, pl.ds(half * SH, SH)], out_ref, own_sem, sx, qx)

    def y_copy(k, dy):
        f = k // SUBS * 2
        src = term.at[f, :, (p.y + dy) % Y, rows_of(k)]
        return remote(src, ry.at[k, dy - 1], sy.at[k, dy - 1], qy.at[k, dy - 1], p.beside(dy))

    def final_copy(k, dy):
        f = k // SUBS * 2 + 1
        src = term.at[f, p.end, (p.y + dy) % Y, rows_of(k)]
        return remote(src, rf.at[k, dy - 1], sf.at[k, dy - 1], qf.at[k, dy - 1], p.beside(dy))

    def wide_copy(k, end):
        f = k // SUBS * 2 + 1
        src = term.at[f, end, :, rows_of(k)]
        if end == 0:
            return remote(src, rd2.at[k], sd2.at[k], qd2.at[k], p.below())
        return remote(src, ru2.at[k], su2.at[k], qu2.at[k], p.above())

    def thin_copy(k, end):
        f = k // SUBS * 2
        src = term.at[f, end, p.y, rows_of(k)]
        if end == 0:
            return remote(src, rd1.at[k], sd1.at[k], qd1.at[k], p.below())
        return remote(src, ru1.at[k], su1.at[k], qu1.at[k], p.above())

    starts = (p.top, p.bottom)
    stops = (p.bottom, p.top)
    hops = (p.down_hops, p.up_hops)
    thin_from, wide_from = (rd1, ru1), (rd2, ru2)

    def step(i):
        if SUBS == 1:
            fresh = i < count
        else:
            fresh = both(i < count, i % SUBS == 0)

        @pl.when(fresh)
        def _():
            f = i // SUBS * 2
            compute(f)
            compute(f + 1)

        @pl.when(i < count)
        def _():
            for dy in range(1, Y):
                y_copy(i, dy).start()
            for end in range(2):

                @pl.when(starts[end])
                def _():
                    wide_copy(i, end).start()

        for end in range(2):
            k = i - hops[end]

            @pl.when(both(jnp.logical_not(starts[end]), within(k, count)))
            def _():
                f = k // SUBS * 2 + 1
                wide_copy(k, end).wait_recv()
                term[f, end, :, rows_of(k)] += wide_from[end][k]

                @pl.when(jnp.logical_not(stops[end]))
                def _():
                    wide_copy(k, end).start()

                @pl.when(stops[end])
                def _():
                    for dy in range(1, Y):
                        final_copy(k, dy).start()

        @pl.when(within(i - 1, count))
        def _():
            k = i - 1
            f = k // SUBS * 2
            for dy in range(1, Y):
                y_copy(k, dy).wait_recv()
                term[f, :, p.y, rows_of(k)] += ry[k, dy - 1]
            for end in range(2):

                @pl.when(starts[end])
                def _():
                    thin_copy(k, end).start()

        for end in range(2):
            k = i - 1 - hops[end]

            @pl.when(both(jnp.logical_not(starts[end]), within(k, count)))
            def _():
                f = k // SUBS * 2
                thin_copy(k, end).wait_recv()
                term[f, end, p.y, rows_of(k)] += thin_from[end][k]

                @pl.when(jnp.logical_not(stops[end]))
                def _():
                    thin_copy(k, end).start()

                @pl.when(stops[end])
                def _():
                    deliver(f, k)

        @pl.when(both(p.corner, within(i - p.Z, count)))
        def _():
            k = i - p.Z
            f = k // SUBS * 2 + 1
            for dy in range(1, Y):
                final_copy(k, dy).wait_recv()
                term[f, p.end, p.y, rows_of(k)] += rf[k, dy - 1]
            deliver(f, k)

    loop(count + p.Z, step)

    def finish(k):
        for dy in range(1, Y):
            y_copy(k, dy).wait_send()
        for end in range(2):

            @pl.when(jnp.logical_not(stops[end]))
            def _():
                wide_copy(k, end).wait_send()
                thin_copy(k, end).wait_send()

        @pl.when(p.corner)
        def _():
            for dy in range(1, Y):
                final_copy(k, dy).wait_send()

    loop(count, finish)

    @pl.when(p.corner)
    def _():
        loop(nf, lambda f: spread_wait(p, f, term.at[f, p.end, p.y, pl.ds(0, SH)], out_ref, own_sem, sx, qx))
        for at in range(H):

            @pl.when(p.unit * H + at != p.rec)
            def _():
                onset_copy(at).wait_recv()

    @pl.when(owner_rec == p.rec)
    def _():
        pltpu.make_async_copy(onset_ref, own_onset_ref.at[pl.ds(0, onset_rows)], so.at[1]).wait()

    @pl.when(owner_rec != p.rec)
    def _():
        onset_copy(0).wait_send()


def adjoint(focus, onset_pairs, real, imag):
    p = Place()
    nf, nr, ns = real.shape
    width = focus.shape[2]
    Y, Z = p.Y, p.Z
    H = Z // 2
    SU = H * nr
    count = nf // 2 * SUBS
    SR, SH = SU // SUBS, SU // CORES
    f32 = jnp.float32
    dma = pltpu.SemaphoreType.DMA
    scratch = [
        pltpu.VMEM((nf, 2, Y, SU, width), f32),
        pltpu.VMEM((2, 2 * nr, ns), f32),
        pltpu.VMEM((count, Y - 1, 2, SR, width), f32),
        pltpu.VMEM((count, SR, width), f32),
        pltpu.VMEM((count, SR, width), f32),
        pltpu.VMEM((count, Y, SR, width), f32),
        pltpu.VMEM((count, Y, SR, width), f32),
        pltpu.VMEM((count, Y - 1, SR, width), f32),
        dma((2, 2)),
        dma((count, Y - 1)),
        dma((count, Y - 1)),
        *[dma((count,))] * 8,
        dma((count, Y - 1)),
        dma((count, Y - 1)),
        dma((nf,)),
        dma((CORES, p.X, nf)),
        dma((p.FQ, nf)),
        dma((2,)),
        dma((H,)),
    ]
    return pl.pallas_call(
        adjoint_kernel,
        out_shape=(
            jax.ShapeDtypeStruct((p.FQ * nf, SH, width), f32),
            jax.ShapeDtypeStruct((H * onset_pairs.shape[0], onset_pairs.shape[1]), jnp.int32),
        ),
        in_specs=[IN_VMEM, ANY, ANY, ANY],
        out_specs=(ANY, ANY),
        scratch_shapes=scratch,
        compiler_params=pltpu.CompilerParams(has_side_effects=True, vmem_limit_bytes=VMEM_LIMIT),
        name="adjoint",
    )(focus.reshape(nr * nf, width), onset_pairs, real, imag)


def forward_kernel(win_ref, real_ref, imag_ref, out_ref, *scratch):
    (full, buf, fo) = scratch[:3]
    (fetch_sem, s0, q0, l0, sy, qy, sd1, qd1, su1, qu1, sd2, qd2, su2, qu2, sf, qf, own_sem, sx, qx) = scratch[3:]
    p = Place()
    nf, _, Y, SU, width = full.shape
    slots = buf.shape[0]
    nr = buf.shape[1] // 2
    half_width = width // 2
    pairs = nf // 2
    count = pairs * SUBS
    SR, SH = SU // SUBS, SU // CORES
    NH = nr // CORES
    U = 2 * Y

    def fetch(f):
        return fetch_response(real_ref, imag_ref, buf, fetch_sem, f)

    for f in range(min(slots, nf)):
        for copy in fetch(f):
            copy.start()

    def own_copy(g):
        rows = pl.ds(p.c * SH, SH)
        return pltpu.make_async_copy(
            win_ref.at[p.c, pl.ds(2 * g, 2)], full.at[pl.ds(2 * g, 2), p.end, p.y, rows], l0.at[g]
        )

    def core_copy(g):
        rows = pl.ds(p.c * SH, SH)
        return remote(
            win_ref.at[1 - p.c, pl.ds(2 * g, 2)],
            full.at[pl.ds(2 * g, 2), p.end, p.y, rows],
            s0.at[g],
            q0.at[g],
            (p.x * CORES + 1 - p.c, p.rec),
        )

    @pl.when(p.corner)
    def _():
        def begin(g):
            core_copy(g).start()
            own_copy(g).start()

        loop(pairs, begin)

    def rows_of(k):
        return pl.ds(k % SUBS * SR, SR)

    def first_y(k, dy, end):
        src = full.at[k // SUBS * 2 + 1, end, p.y, rows_of(k)]
        return remote(src, src, sf.at[k, dy - 1], qf.at[k, dy - 1], p.beside(dy))

    def last_y(k, dy, end):
        src = full.at[k // SUBS * 2, end, p.y, rows_of(k)]
        return remote(src, src, sy.at[end, k, dy - 1], qy.at[end, k, dy - 1], p.beside(dy))

    def thin_copy(k, end):
        src = full.at[k // SUBS * 2, end, p.y, rows_of(k)]
        if end == 0:
            return remote(src, src, su1.at[k], qu1.at[k], p.above())
        return remote(src, src, sd1.at[k], qd1.at[k], p.below())

    def wide_copy(k, end):
        src = full.at[k // SUBS * 2 + 1, end, :, rows_of(k)]
        if end == 0:
            return remote(src, src, su2.at[k], qu2.at[k], p.above())
        return remote(src, src, sd2.at[k], qd2.at[k], p.below())

    starts = (p.bottom, p.top)
    stops = (p.top, p.bottom)
    hops = (p.up_hops, p.down_hops)

    def compute(f):
        for copy in fetch(f):
            copy.wait()
        slot = f % slots
        total = None
        for u in range(U):
            high, low = split(buf[slot, :, u * SU : (u + 1) * SU])
            f_high, f_low = split(full[f, u // Y, u % Y])
            wide = jnp.dot(
                high, jnp.concatenate([f_high, f_low], axis=1), preferred_element_type=jnp.float32
            )
            rest = jnp.dot(low, f_high, preferred_element_type=jnp.float32)
            piece = wide[:, :width] + wide[:, width:] + rest
            total = piece if total is None else total + piece
        turned = pltpu.roll(total[nr:], half_width, 1)
        lane = lax.broadcasted_iota(jnp.int32, (1, width), 1)
        fo[f] = total[:nr] + jnp.where(lane < half_width, -turned, turned)

        @pl.when(f + slots < nf)
        def _():
            for copy in fetch(f + slots):
                copy.start()

    def deliver(f):
        for half in range(CORES):
            spread(p, f, half, fo.at[f, pl.ds(half * NH, NH)], out_ref, own_sem, sx, qx)

    def step(i):
        @pl.when(both(p.corner, i < count))
        def _():
            if SUBS == 1:
                fresh = i >= 0
            else:
                fresh = i % SUBS == 0

            @pl.when(fresh)
            def _():
                own_copy(i // SUBS).wait()
                core_copy(i // SUBS).wait_recv()

            for end in range(2):

                @pl.when(starts[end])
                def _():
                    for dy in range(1, Y):
                        first_y(i, dy, end).start()

        for end in range(2):
            k = i - hops[end]

            @pl.when(within(k, count))
            def _():
                @pl.when(jnp.logical_not(starts[end]))
                def _():
                    thin_copy(k, end).wait_recv()

                @pl.when(jnp.logical_not(stops[end]))
                def _():
                    thin_copy(k, end).start()

                for dy in range(1, Y):
                    last_y(k, dy, end).start()

            j = i - 1 - hops[end]

            @pl.when(within(j, count))
            def _():
                @pl.when(starts[end])
                def _():
                    for dy in range(1, Y):
                        first_y(j, dy, end).wait_recv()

                @pl.when(jnp.logical_not(starts[end]))
                def _():
                    wide_copy(j, end).wait_recv()

                @pl.when(jnp.logical_not(stops[end]))
                def _():
                    wide_copy(j, end).start()

        k = i - p.Z

        @pl.when(within(k, count))
        def _():
            for end in range(2):
                for dy in range(1, Y):
                    last_y(k, dy, end).wait_recv()

            if SUBS == 1:
                ready = k >= 0
            else:
                ready = k % SUBS == SUBS - 1

            @pl.when(ready)
            def _():
                f = k // SUBS * 2
                compute(f)
                deliver(f)
                compute(f + 1)
                deliver(f + 1)

    loop(count + p.Z, step)

    def finish(k):
        for end in range(2):
            for dy in range(1, Y):
                last_y(k, dy, end).wait_send()

            @pl.when(jnp.logical_not(stops[end]))
            def _():
                thin_copy(k, end).wait_send()
                wide_copy(k, end).wait_send()

            @pl.when(starts[end])
            def _():
                for dy in range(1, Y):
                    first_y(k, dy, end).wait_send()

    loop(count, finish)

    @pl.when(p.corner)
    def _():
        loop(pairs, lambda g: core_copy(g).wait_send())

    loop(nf, lambda f: spread_wait(p, f, fo.at[f, pl.ds(0, NH)], out_ref, own_sem, sx, qx))


def forward(windowed, real, imag):
    p = Place()
    nf, nr, ns = real.shape
    width = windowed.shape[3]
    Y, Z = p.Y, p.Z
    SU = Z // 2 * nr
    count = nf // 2 * SUBS
    f32 = jnp.float32
    dma = pltpu.SemaphoreType.DMA
    scratch = [
        pltpu.VMEM((nf, 2, Y, SU, width), f32),
        pltpu.VMEM((4, 2 * nr, ns), f32),
        pltpu.VMEM((nf, nr, width), f32),
        dma((4, 2)),
        dma((nf // 2,)),
        dma((nf // 2,)),
        dma((nf // 2,)),
        dma((2, count, Y - 1)),
        dma((2, count, Y - 1)),
        *[dma((count,))] * 8,
        dma((count, Y - 1)),
        dma((count, Y - 1)),
        dma((nf,)),
        dma((CORES, p.X, nf)),
        dma((p.FQ, nf)),
    ]
    return pl.pallas_call(
        forward_kernel,
        out_shape=jax.ShapeDtypeStruct((p.FQ * nf, nr // CORES, width), f32),
        in_specs=[ANY, ANY, ANY],
        out_specs=ANY,
        scratch_shapes=scratch,
        compiler_params=pltpu.CompilerParams(has_side_effects=True, vmem_limit_bytes=VMEM_LIMIT),
        name="forward",
    )(windowed, real, imag)


def split_host(table):
    high = np.asarray(table, dtype=jnp.bfloat16)
    low = np.asarray(table - high.astype(np.float64), dtype=jnp.bfloat16)
    return high, low


def tables(freqs):
    samples = 2 * freqs
    order = np.arange(freqs)
    sample = np.arange(samples)
    phases = 2.0 * math.pi / samples * (order[:, None] * sample[None, :] % samples)
    cosine, sine = np.cos(phases), np.sin(phases)
    factor = np.where(order == 0, 1.0, 2.0)[:, None] / samples
    inverse = np.concatenate([(factor * cosine).T, (-factor * sine).T], axis=1)
    return (*split_host(inverse), *split_host(cosine), *split_host(-sine))


def triple(high, low, x):
    x_high, x_low = split(x)
    dot = functools.partial(jnp.dot, preferred_element_type=jnp.float32)
    return dot(high, x_high) + (dot(high, x_low) + dot(low, x_high))


def window_kernel(by_row, onset_ref, ih_ref, il_ref, fh_ref, fl_ref, x_ref, o_ref):
    freqs, rows, width = x_ref.shape
    samples = 2 * freqs
    half = width // 2
    kept = fh_ref.shape[0] // 2
    own = kept // CORES
    first = lax.broadcasted_iota(jnp.int32, (1, width), 1) < half
    sample = lax.broadcasted_iota(jnp.int32, (samples, width), 0)
    pairs = rows // 2
    packed = []
    for i in range(pairs):
        a, b = x_ref[:, 2 * i, :], x_ref[:, 2 * i + 1, :]
        real = jnp.where(first, a, pltpu.roll(b, half, 1))
        imag = jnp.where(first, pltpu.roll(a, half, 1), b)
        packed.append(jnp.concatenate([real, imag], axis=0))
    traces = triple(ih_ref[...], il_ref[...], jnp.concatenate(packed, axis=1))
    clipped = [
        jnp.where(sample < onset_ref[0, i : i + 1, :], traces[:, i * width : (i + 1) * width], 0.0)
        for i in range(pairs)
    ]
    back = triple(fh_ref[...], fl_ref[...], jnp.concatenate(clipped, axis=1))
    for i in range(pairs):
        real = back[:kept, i * width : (i + 1) * width]
        imag = back[kept:, i * width : (i + 1) * width]
        a = jnp.where(first, real, pltpu.roll(imag, half, 1))
        b = jnp.where(first, pltpu.roll(real, half, 1), imag)
        for n, value in ((2 * i, a), (2 * i + 1, b)):
            for core in range(CORES):
                piece = value[core * own : (core + 1) * own]
                if by_row:
                    o_ref[core, n] = piece
                else:
                    o_ref[core, :, n, :] = piece


def window(spectrum, onset_pairs, consts, by_row):
    freqs, count, width = spectrum.shape
    own = consts[2].shape[0] // 2 // CORES
    rows = 8
    onset_pairs = onset_pairs.reshape(count // rows, rows // 2, width)
    whole = [pl.BlockSpec(t.shape, lambda i: (0, 0)) for t in consts]
    if by_row:
        out_shape, out_block = (CORES, count, own, width), (CORES, rows, own, width)
        out_spec = pl.BlockSpec(out_block, lambda i: (0, i, 0, 0))
    else:
        out_shape, out_block = (CORES, own, count, width), (CORES, own, rows, width)
        out_spec = pl.BlockSpec(out_block, lambda i: (0, 0, i, 0))
    return pl.pallas_call(
        functools.partial(window_kernel, by_row),
        grid=(count // rows,),
        in_specs=[
            pl.BlockSpec((1, rows // 2, width), lambda i: (i, 0, 0)),
            *whole,
            pl.BlockSpec((freqs, rows, width), lambda i: (0, i, 0)),
        ],
        out_specs=out_spec,
        out_shape=jax.ShapeDtypeStruct(out_shape, jnp.float32),
        name="window_rows" if by_row else "window",
    )(onset_pairs, *consts, spectrum)


def on_device(response_real, response_imaginary, focus, initial, onset):
    p = Place()
    nf, nr, _ = response_real.shape
    width = focus.shape[2]
    onset_pairs = onset.reshape(nr // 2, width)

    inv_high, inv_low, cos_high, cos_low, sin_high, sin_low = tables(p.FQ * nf)

    def chip_rows(cosine, sine):
        at = p.x * CORES * nf
        cut = [lax.dynamic_slice_in_dim(jnp.asarray(t), at, CORES * nf, 0) for t in (cosine, sine)]
        return jnp.concatenate(cut, axis=0)

    consts = [jnp.asarray(inv_high), jnp.asarray(inv_low), chip_rows(cos_high, sin_high), chip_rows(cos_low, sin_low)]

    spectrum, own_onset = adjoint(focus, onset_pairs, response_real, response_imaginary)
    SH = spectrum.shape[1]
    mine = lax.dynamic_slice_in_dim(own_onset, p.c * (SH // 2), SH // 2, 0)
    windowed = window(spectrum, mine, consts, False)
    received = forward(windowed, response_real, response_imaginary)
    quarter = nr // CORES // 2
    mine = lax.dynamic_slice_in_dim(onset_pairs, p.c * quarter, quarter, 0)
    update = window(received, mine, consts, True)
    keep = lax.dynamic_index_in_dim(update, p.c, 0, keepdims=False)
    give = lax.dynamic_index_in_dim(update, 1 - p.c, 0, keepdims=False)
    swap = [(i, i ^ 1) for i in range(p.FQ)]
    got = lax.ppermute(give, "freq", swap)
    low = jnp.where(p.c == 0, keep, got)
    high = jnp.where(p.c == 0, got, keep)
    return initial - jnp.concatenate([low, high], axis=0)


def solution(mesh):
    return jax.shard_map(
        on_device,
        mesh=mesh,
        in_specs=(
            P("freq", "rec", None),
            P("freq", "rec", None),
            P("rec", "freq", None),
            P("rec", "freq", None),
            P("rec", None),
        ),
        out_specs=P("rec", "freq", None),
        check_vma=False,
    )
```

```python
import functools
import math

import jax
import jax.numpy as jnp
import numpy as np
from jax import lax
from jax.experimental import pallas as pl
from jax.experimental.pallas import tpu as pltpu
from jax.sharding import PartitionSpec as P

CORES = 2
SUBS = 2
VMEM_LIMIT = 63 * 2**20
MESH = pl.DeviceIdType.MESH
ANY = pl.BlockSpec(memory_space=pl.ANY)
IN_VMEM = pl.BlockSpec(memory_space=pltpu.VMEM)


class Place:
    def __init__(self):
        total = lax.axis_size("rec")
        ys = 1 << ((total.bit_length() - 1) // 2)
        self.Y = ys if total % ys == 0 else 1
        self.Z = total // self.Y
        self.FQ = lax.axis_size("freq")
        self.X = self.FQ // CORES
        self.rec = lax.axis_index("rec")
        self.freq = lax.axis_index("freq")
        self.z, self.y = self.rec // self.Y, self.rec % self.Y
        self.x, self.c = self.freq // CORES, self.freq % CORES
        self.down_hops, self.up_hops = self.Z - 1 - self.z, self.z
        self.bottom, self.top = self.z == 0, self.z == self.Z - 1
        self.corner = jnp.logical_or(self.bottom, self.top)
        self.end = jnp.where(self.bottom, 0, 1)
        self.unit = self.end * self.Y + self.y

    def above(self):
        return (self.freq, self.rec + self.Y)

    def below(self):
        return (self.freq, self.rec - self.Y)

    def beside(self, dy):
        return (self.freq, self.z * self.Y + (self.y + dy) % self.Y)


def remote(src, dst, send, recv, device):
    return pltpu.make_async_remote_copy(src, dst, send, recv, device_id=device, device_id_type=MESH)


def within(k, count):
    return jnp.logical_and(k >= 0, k < count)


def both(a, b):
    return jnp.logical_and(a, b)


def split(x):
    high = x.astype(jnp.bfloat16)
    return high, (x - high.astype(jnp.float32)).astype(jnp.bfloat16)


def loop(count, body):
    lax.fori_loop(0, count, lambda k, _: (body(k), 0)[1], 0)


def partners(p):
    found = [(p.z < p.Z - 1, p.above()), (p.z > 0, p.below())]
    found += [(p.z >= 0, p.beside(dy)) for dy in range(1, p.Y)]
    for step in range(1, p.FQ):
        found.append((p.z >= 0, ((p.freq + step) % p.FQ, p.rec)))
    return found


def greet(found):
    barrier = pltpu.get_barrier_semaphore()
    for wanted, device in found:

        @pl.when(wanted)
        def _():
            pl.semaphore_signal(barrier, inc=1, device_id=device, device_id_type=MESH)


def meet(found):
    total = sum(wanted.astype(jnp.int32) for wanted, _ in found)
    pl.semaphore_wait(pltpu.get_barrier_semaphore(), total)


def fetch_response(real_ref, imag_ref, buf, sems, f):
    slots = buf.shape[0]
    rows = buf.shape[1] // 2
    slot = f % slots
    return [
        pltpu.make_async_copy(ref.at[f], buf.at[slot, pl.ds(k * rows, rows)], sems.at[slot, k])
        for k, ref in enumerate((real_ref, imag_ref))
    ]


def spread(p, half, src, dst, own, send, recv):
    for dx in range(p.X):
        copy = remote(src, dst, send(dx), recv, ((p.x + dx) % p.X * CORES + half, p.rec))
        if dx == 0:

            @pl.when(p.c == half)
            def _():
                pltpu.make_async_copy(src, dst, own).start()

            @pl.when(p.c != half)
            def _():
                copy.start()
        else:
            copy.start()


def spread_sent(p, half, src, dst, own, send):
    for dx in range(p.X):
        copy = remote(src, dst, send(dx), own, (p.freq, p.rec))
        if dx == 0:

            @pl.when(p.c == half)
            def _():
                pltpu.make_async_copy(src, dst, own).wait()

            @pl.when(p.c != half)
            def _():
                copy.wait_send()
        else:
            copy.wait_send()


def adjoint_kernel(focus_ref, onset_ref, real_ref, imag_ref, out_ref, own_onset_ref, *scratch):
    (term, buf, ry, rd1, ru1, rd2, ru2, rf) = scratch[:8]
    (fetch_sem, sy, qy, sd1, qd1, su1, qu1, sd2, qd2, su2, qu2, sf, qf, own_sem, sx, qx, so, qo) = scratch[8:]
    p = Place()
    nf, _, Y, SU, width = term.shape
    slots = buf.shape[0]
    pairs = nf // 2
    count = pairs * SUBS
    SR, SH = SU // SUBS, SU // CORES
    H = p.Z // 2
    U = 2 * Y
    per_half = SUBS // CORES
    nr = buf.shape[1] // 2
    sign = jnp.where(lax.broadcasted_iota(jnp.int32, (1, width), 1) < width // 2, 1.0, -1.0)

    def fetch(f):
        return fetch_response(real_ref, imag_ref, buf, fetch_sem, f)

    owner = p.rec // H
    owner_rec = owner // Y * (p.Z - 1) * Y + owner % Y
    onset_rows = onset_ref.shape[0]

    def onset_copy(at):
        dst = own_onset_ref.at[pl.ds(at * onset_rows, onset_rows)]
        return remote(onset_ref, dst, so.at[0], qo.at[at], (p.freq, owner_rec))

    found = partners(p)
    found.append((owner_rec != p.rec, (p.freq, owner_rec)))
    for at in range(H):
        giver = p.unit * H + at
        found.append((both(p.corner, giver != p.rec), (p.freq, giver)))
    greet(found)
    for f in range(min(slots, nf)):
        for copy in fetch(f):
            copy.start()

    def compute(f):
        for copy in fetch(f):
            copy.wait()
        slot = f % slots
        x = focus_ref[pl.ds(f, nr, stride=nf), :]
        crossed = pltpu.roll(x, width // 2, 1) * sign
        z_high, z_low = split(jnp.concatenate([x, crossed], axis=0).T)
        z = jnp.concatenate([z_high, z_low], axis=0)
        for u in range(0, U, 2):
            high, low = split(buf[slot, :, u * SU : (u + 2) * SU])
            wide = jnp.dot(z, high, preferred_element_type=jnp.float32)
            rest = jnp.dot(z_high, low, preferred_element_type=jnp.float32)
            total = wide[:width] + wide[width:] + rest
            term[f, u // Y, u % Y : u % Y + 2] = total.T.reshape(2, SU, width)

        @pl.when(f + slots < nf)
        def _():
            for copy in fetch(f + slots):
                copy.start()

    def rows_of(k):
        return pl.ds(k % SUBS * SR, SR)

    def portion(f, sub):
        half, at = sub // per_half, sub % per_half
        src = term.at[f, p.end, p.y, pl.ds(sub * SR, SR)]
        dst = out_ref.at[p.freq * nf + f, pl.ds(at * SR, SR)]
        slot = f * per_half + at
        return half, src, dst, own_sem.at[slot], lambda dx: sx.at[half, dx, slot], qx.at[p.freq, slot]

    def deliver(f, k):
        spread(p, *portion(f, k % SUBS))

    def y_copy(k, dy):
        f = k // SUBS * 2
        src = term.at[f, :, (p.y + dy) % Y, rows_of(k)]
        return remote(src, ry.at[k, dy - 1], sy.at[k, dy - 1], qy.at[k, dy - 1], p.beside(dy))

    def final_copy(k, dy):
        f = k // SUBS * 2 + 1
        src = term.at[f, p.end, (p.y + dy) % Y, rows_of(k)]
        return remote(src, rf.at[k, dy - 1], sf.at[k, dy - 1], qf.at[k, dy - 1], p.beside(dy))

    def wide_copy(k, end):
        f = k // SUBS * 2 + 1
        src = term.at[f, end, :, rows_of(k)]
        if end == 0:
            return remote(src, rd2.at[k], sd2.at[k], qd2.at[k], p.below())
        return remote(src, ru2.at[k], su2.at[k], qu2.at[k], p.above())

    def thin_copy(k, end):
        f = k // SUBS * 2
        src = term.at[f, end, p.y, rows_of(k)]
        if end == 0:
            return remote(src, rd1.at[k], sd1.at[k], qd1.at[k], p.below())
        return remote(src, ru1.at[k], su1.at[k], qu1.at[k], p.above())

    starts = (p.top, p.bottom)
    stops = (p.bottom, p.top)
    hops = (p.down_hops, p.up_hops)
    thin_from, wide_from = (rd1, ru1), (rd2, ru2)

    def begin(k):
        for dy in range(1, Y):
            y_copy(k, dy).start()
        for end in range(2):

            @pl.when(starts[end])
            def _():
                wide_copy(k, end).start()

    compute(0)
    compute(1)
    meet(found)
    @pl.when(owner_rec == p.rec)
    def _():
        at = p.rec % H
        pltpu.make_async_copy(onset_ref, own_onset_ref.at[pl.ds(at * onset_rows, onset_rows)], so.at[1]).start()

    @pl.when(owner_rec != p.rec)
    def _():
        onset_copy(p.rec % H).start()

    begin(0)

    def step(i):
        @pl.when(i + 2 < nf)
        def _():
            compute(i + 2)

        @pl.when(i + 1 < count)
        def _():
            begin(i + 1)

        for end in range(2):
            k = i - hops[end]

            @pl.when(both(jnp.logical_not(starts[end]), within(k, count)))
            def _():
                f = k // SUBS * 2 + 1
                wide_copy(k, end).wait_recv()
                term[f, end, :, rows_of(k)] += wide_from[end][k]

                @pl.when(jnp.logical_not(stops[end]))
                def _():
                    wide_copy(k, end).start()

                @pl.when(stops[end])
                def _():
                    for dy in range(1, Y):
                        final_copy(k, dy).start()

        @pl.when(within(i - 1, count))
        def _():
            k = i - 1
            f = k // SUBS * 2
            for dy in range(1, Y):
                y_copy(k, dy).wait_recv()
                term[f, :, p.y, rows_of(k)] += ry[k, dy - 1]
            for end in range(2):

                @pl.when(starts[end])
                def _():
                    thin_copy(k, end).start()

        for end in range(2):
            k = i - 1 - hops[end]

            @pl.when(both(jnp.logical_not(starts[end]), within(k, count)))
            def _():
                f = k // SUBS * 2
                thin_copy(k, end).wait_recv()
                term[f, end, p.y, rows_of(k)] += thin_from[end][k]

                @pl.when(jnp.logical_not(stops[end]))
                def _():
                    thin_copy(k, end).start()

                @pl.when(stops[end])
                def _():
                    deliver(f, k)

        @pl.when(both(p.corner, within(i - p.Z, count)))
        def _():
            k = i - p.Z
            f = k // SUBS * 2 + 1
            for dy in range(1, Y):
                final_copy(k, dy).wait_recv()
                term[f, p.end, p.y, rows_of(k)] += rf[k, dy - 1]
            deliver(f, k)

    loop(count + p.Z, step)

    def finish(k):
        for dy in range(1, Y):
            y_copy(k, dy).wait_send()
        for end in range(2):

            @pl.when(jnp.logical_not(stops[end]))
            def _():
                wide_copy(k, end).wait_send()
                thin_copy(k, end).wait_send()

        @pl.when(p.corner)
        def _():
            for dy in range(1, Y):
                final_copy(k, dy).wait_send()

    loop(count, finish)

    @pl.when(p.corner)
    def _():
        def settle(f):
            for sub in range(SUBS):
                spread_sent(p, *portion(f, sub)[:-1])
            for source in range(p.FQ):

                @pl.when(p.freq != source)
                def _():
                    for at in range(per_half):
                        src = term.at[f, p.end, p.y, pl.ds(0, SR)]
                        dst = out_ref.at[source * nf + f, pl.ds(at * SR, SR)]
                        slot = f * per_half + at
                        remote(src, dst, sx.at[0, 0, slot], qx.at[source, slot], (p.freq, p.rec)).wait_recv()

        loop(nf, settle)
        for at in range(H):

            @pl.when(p.unit * H + at != p.rec)
            def _():
                onset_copy(at).wait_recv()

    @pl.when(owner_rec == p.rec)
    def _():
        pltpu.make_async_copy(onset_ref, own_onset_ref.at[pl.ds(0, onset_rows)], so.at[1]).wait()

    @pl.when(owner_rec != p.rec)
    def _():
        onset_copy(0).wait_send()


def adjoint(focus, onset_pairs, real, imag):
    p = Place()
    nf, nr, ns = real.shape
    width = focus.shape[2]
    Y, Z = p.Y, p.Z
    H = Z // 2
    SU = H * nr
    count = nf // 2 * SUBS
    SR, SH = SU // SUBS, SU // CORES
    f32 = jnp.float32
    dma = pltpu.SemaphoreType.DMA
    scratch = [
        pltpu.VMEM((nf, 2, Y, SU, width), f32),
        pltpu.VMEM((2, 2 * nr, ns), f32),
        pltpu.VMEM((count, Y - 1, 2, SR, width), f32),
        pltpu.VMEM((count, SR, width), f32),
        pltpu.VMEM((count, SR, width), f32),
        pltpu.VMEM((count, Y, SR, width), f32),
        pltpu.VMEM((count, Y, SR, width), f32),
        pltpu.VMEM((count, Y - 1, SR, width), f32),
        dma((2, 2)),
        dma((count, Y - 1)),
        dma((count, Y - 1)),
        *[dma((count,))] * 8,
        dma((count, Y - 1)),
        dma((count, Y - 1)),
        dma((nf * SUBS // CORES,)),
        dma((CORES, p.X, nf * SUBS // CORES)),
        dma((p.FQ, nf * SUBS // CORES)),
        dma((2,)),
        dma((H,)),
    ]
    return pl.pallas_call(
        adjoint_kernel,
        out_shape=(
            jax.ShapeDtypeStruct((p.FQ * nf, SH, width), f32),
            jax.ShapeDtypeStruct((H * onset_pairs.shape[0], onset_pairs.shape[1]), jnp.int32),
        ),
        in_specs=[IN_VMEM, ANY, ANY, ANY],
        out_specs=(ANY, ANY),
        scratch_shapes=scratch,
        compiler_params=pltpu.CompilerParams(
            collective_id=1, has_side_effects=True, vmem_limit_bytes=VMEM_LIMIT
        ),
        name="adjoint",
    )(focus.reshape(nr * nf, width), onset_pairs, real, imag)


def forward_kernel(win_ref, real_ref, imag_ref, out_ref, *scratch):
    (full, buf, fo) = scratch[:3]
    (fetch_sem, s0, q0, l0, sy, qy, sd1, qd1, su1, qu1, sd2, qd2, su2, qu2, sf, qf, own_sem, sx, qx) = scratch[3:]
    p = Place()
    nf, _, Y, SU, width = full.shape
    slots = buf.shape[0]
    nr = buf.shape[1] // 2
    half_width = width // 2
    pairs = nf // 2
    count = pairs * SUBS
    SR, SH = SU // SUBS, SU // CORES
    NH = nr // CORES
    U = 2 * Y

    def fetch(f):
        return fetch_response(real_ref, imag_ref, buf, fetch_sem, f)

    found = partners(p)
    greet(found)
    for f in range(min(slots, nf)):
        for copy in fetch(f):
            copy.start()

    def own_copy(g):
        rows = pl.ds(p.c * SH, SH)
        return pltpu.make_async_copy(
            win_ref.at[p.c, pl.ds(2 * g, 2)], full.at[pl.ds(2 * g, 2), p.end, p.y, rows], l0.at[g]
        )

    def core_copy(g):
        rows = pl.ds(p.c * SH, SH)
        return remote(
            win_ref.at[1 - p.c, pl.ds(2 * g, 2)],
            full.at[pl.ds(2 * g, 2), p.end, p.y, rows],
            s0.at[g],
            q0.at[g],
            (p.x * CORES + 1 - p.c, p.rec),
        )

    @pl.when(p.corner)
    def _():
        loop(pairs, lambda g: own_copy(g).start())

    meet(found)

    @pl.when(p.corner)
    def _():
        loop(pairs, lambda g: core_copy(g).start())

    def rows_of(k):
        return pl.ds(k % SUBS * SR, SR)

    def first_y(k, dy, end):
        src = full.at[k // SUBS * 2 + 1, end, p.y, rows_of(k)]
        return remote(src, src, sf.at[k, dy - 1], qf.at[k, dy - 1], p.beside(dy))

    def last_y(k, dy, end):
        src = full.at[k // SUBS * 2, end, p.y, rows_of(k)]
        return remote(src, src, sy.at[end, k, dy - 1], qy.at[end, k, dy - 1], p.beside(dy))

    def thin_copy(k, end):
        src = full.at[k // SUBS * 2, end, p.y, rows_of(k)]
        if end == 0:
            return remote(src, src, su1.at[k], qu1.at[k], p.above())
        return remote(src, src, sd1.at[k], qd1.at[k], p.below())

    def wide_copy(k, end):
        src = full.at[k // SUBS * 2 + 1, end, :, rows_of(k)]
        if end == 0:
            return remote(src, src, su2.at[k], qu2.at[k], p.above())
        return remote(src, src, sd2.at[k], qd2.at[k], p.below())

    starts = (p.bottom, p.top)
    stops = (p.top, p.bottom)
    hops = (p.up_hops, p.down_hops)

    def compute(f):
        for copy in fetch(f):
            copy.wait()
        slot = f % slots
        total = None
        for u in range(U):
            high, low = split(buf[slot, :, u * SU : (u + 1) * SU])
            f_high, f_low = split(full[f, u // Y, u % Y])
            wide = jnp.dot(
                high, jnp.concatenate([f_high, f_low], axis=1), preferred_element_type=jnp.float32
            )
            rest = jnp.dot(low, f_high, preferred_element_type=jnp.float32)
            piece = wide[:, :width] + wide[:, width:] + rest
            total = piece if total is None else total + piece
        turned = pltpu.roll(total[nr:], half_width, 1)
        lane = lax.broadcasted_iota(jnp.int32, (1, width), 1)
        fo[f] = total[:nr] + jnp.where(lane < half_width, -turned, turned)

        @pl.when(f + slots < nf)
        def _():
            for copy in fetch(f + slots):
                copy.start()

    def portion(f, half):
        src = fo.at[f, pl.ds(half * NH, NH)]
        dst = out_ref.at[p.freq * nf + f]
        return half, src, dst, own_sem.at[f], lambda dx: sx.at[half, dx, f], qx.at[p.freq, f]

    def deliver(f):
        for half in range(CORES):
            spread(p, *portion(f, half))

    def begin(k):
        for end in range(2):

            @pl.when(starts[end])
            def _():
                for dy in range(1, Y):
                    first_y(k, dy, end).start()
                thin_copy(k, end).start()

    @pl.when(p.corner)
    def _():
        own_copy(0).wait()
        core_copy(0).wait_recv()
        begin(0)

    def step(i):
        @pl.when(both(p.corner, i + 1 < count))
        def _():
            @pl.when((i + 1) % SUBS == 0)
            def _():
                own_copy((i + 1) // SUBS).wait()
                core_copy((i + 1) // SUBS).wait_recv()

            begin(i + 1)

        for end in range(2):
            k = i - hops[end]

            @pl.when(within(k, count))
            def _():
                @pl.when(jnp.logical_not(starts[end]))
                def _():
                    thin_copy(k, end).wait_recv()

                @pl.when(jnp.logical_not(jnp.logical_or(starts[end], stops[end])))
                def _():
                    thin_copy(k, end).start()

                for dy in range(1, Y):
                    last_y(k, dy, end).start()

            j = i - 1 - hops[end]

            @pl.when(within(j, count))
            def _():
                @pl.when(starts[end])
                def _():
                    for dy in range(1, Y):
                        first_y(j, dy, end).wait_recv()

                @pl.when(jnp.logical_not(starts[end]))
                def _():
                    wide_copy(j, end).wait_recv()

                @pl.when(jnp.logical_not(stops[end]))
                def _():
                    wide_copy(j, end).start()

        k = i - p.Z

        @pl.when(within(k, count))
        def _():
            for end in range(2):
                for dy in range(1, Y):
                    last_y(k, dy, end).wait_recv()

        f = k - SUBS + 1

        @pl.when(within(f, nf))
        def _():
            compute(f)
            deliver(f)

    loop(count + p.Z + SUBS - 1, step)

    def finish(k):
        for end in range(2):
            for dy in range(1, Y):
                last_y(k, dy, end).wait_send()

            @pl.when(jnp.logical_not(stops[end]))
            def _():
                thin_copy(k, end).wait_send()
                wide_copy(k, end).wait_send()

            @pl.when(starts[end])
            def _():
                for dy in range(1, Y):
                    first_y(k, dy, end).wait_send()

    loop(count, finish)

    @pl.when(p.corner)
    def _():
        loop(pairs, lambda g: core_copy(g).wait_send())

    def settle(f):
        for half in range(CORES):
            spread_sent(p, *portion(f, half)[:-1])
        for source in range(p.FQ):

            @pl.when(p.freq != source)
            def _():
                src = fo.at[f, pl.ds(0, NH)]
                dst = out_ref.at[source * nf + f]
                remote(src, dst, sx.at[0, 0, f], qx.at[source, f], (p.freq, p.rec)).wait_recv()

    loop(nf, settle)


def forward(windowed, real, imag):
    p = Place()
    nf, nr, ns = real.shape
    width = windowed.shape[3]
    Y, Z = p.Y, p.Z
    SU = Z // 2 * nr
    count = nf // 2 * SUBS
    f32 = jnp.float32
    dma = pltpu.SemaphoreType.DMA
    scratch = [
        pltpu.VMEM((nf, 2, Y, SU, width), f32),
        pltpu.VMEM((4, 2 * nr, ns), f32),
        pltpu.VMEM((nf, nr, width), f32),
        dma((4, 2)),
        dma((nf // 2,)),
        dma((nf // 2,)),
        dma((nf // 2,)),
        dma((2, count, Y - 1)),
        dma((2, count, Y - 1)),
        *[dma((count,))] * 8,
        dma((count, Y - 1)),
        dma((count, Y - 1)),
        dma((nf,)),
        dma((CORES, p.X, nf)),
        dma((p.FQ, nf)),
    ]
    return pl.pallas_call(
        forward_kernel,
        out_shape=jax.ShapeDtypeStruct((p.FQ * nf, nr // CORES, width), f32),
        in_specs=[ANY, ANY, ANY],
        out_specs=ANY,
        scratch_shapes=scratch,
        compiler_params=pltpu.CompilerParams(
            collective_id=2, has_side_effects=True, vmem_limit_bytes=VMEM_LIMIT
        ),
        name="forward",
    )(windowed, real, imag)


def stack_host(table):
    high = np.asarray(table, dtype=jnp.bfloat16)
    low = np.asarray(table - high.astype(np.float64), dtype=jnp.bfloat16)
    return np.concatenate([high, low], axis=-2)


def tables(freqs, chips):
    samples = 2 * freqs
    order = np.arange(freqs)
    sample = np.arange(samples)
    phases = 2.0 * math.pi / samples * (order[:, None] * sample[None, :] % samples)
    cosine, sine = np.cos(phases), np.sin(phases)
    factor = np.where(order == 0, 1.0, 2.0)[:, None] / samples
    inverse = np.concatenate([(factor * cosine).T, (-factor * sine).T], axis=1)
    shape = (chips, freqs // chips, samples)
    forward = np.concatenate([cosine.reshape(shape), -sine.reshape(shape)], axis=1)
    return jnp.asarray(stack_host(inverse)), jnp.asarray(stack_host(forward))


def triple(stack, x):
    high, low = split(x)
    dot = functools.partial(jnp.dot, preferred_element_type=jnp.float32)
    rows = stack.shape[0] // 2
    wide = dot(stack, high)
    return wide[:rows] + (wide[rows:] + dot(stack[:rows], low))


def window_rows(inverse, forward, onset_ref, x_ref, start, count, store):
    freqs, _, width = x_ref.shape
    half = width // 2
    samples = 2 * freqs
    kept = forward.shape[0] // 4
    pairs = count // 2
    first = lax.broadcasted_iota(jnp.int32, (1, width), 1) < half
    sample = lax.broadcasted_iota(jnp.int32, (samples, width), 0)
    packed = []
    for i in range(pairs):
        a, b = x_ref[:, start + 2 * i, :], x_ref[:, start + 2 * i + 1, :]
        real = jnp.where(first, a, pltpu.roll(b, half, 1))
        imag = jnp.where(first, pltpu.roll(a, half, 1), b)
        packed.append(jnp.concatenate([real, imag], axis=0))
    traces = triple(inverse, jnp.concatenate(packed, axis=1))
    clipped = []
    for i in range(pairs):
        onset = onset_ref[start // 2 + i : start // 2 + i + 1, :]
        clipped.append(jnp.where(sample < onset, traces[:, i * width : (i + 1) * width], 0.0))
    back = triple(forward, jnp.concatenate(clipped, axis=1))
    for i in range(pairs):
        real = back[:kept, i * width : (i + 1) * width]
        imag = back[kept:, i * width : (i + 1) * width]
        store(start + 2 * i, jnp.where(first, real, pltpu.roll(imag, half, 1)))
        store(start + 2 * i + 1, jnp.where(first, pltpu.roll(real, half, 1), imag))


def groups(rows):
    step = 16 if rows % 16 == 0 else 8
    return [(start, step) for start in range(0, rows, step)]


def rows_per_step(count):
    for rows in (48, 32):
        if count % rows == 0:
            return rows
    return 8


def source_window_kernel(onset_ref, inverse_ref, forward_ref, x_ref, o_ref):
    p = Place()
    rows = x_ref.shape[1]
    own = o_ref.shape[1]
    onsets = onset_ref.at[p.c * pl.num_programs(0) + pl.program_id(0)]
    inverse, forward_table = inverse_ref[...], forward_ref[p.x]

    def store(n, value):
        for core in range(CORES):
            o_ref[core, :, n, :] = value[core * own : (core + 1) * own]

    for start, count in groups(rows):
        window_rows(inverse, forward_table, onsets, x_ref, start, count, store)


def source_window(spectrum, onset_pairs, inverse, forward_table):
    freqs, count, width = spectrum.shape
    own = forward_table.shape[1] // 4 // CORES
    rows = rows_per_step(count)
    steps = count // rows
    onset_pairs = onset_pairs.reshape(CORES * steps, rows // 2, width)
    return pl.pallas_call(
        source_window_kernel,
        grid=(steps,),
        in_specs=[
            *[IN_VMEM] * 3,
            pl.BlockSpec((freqs, rows, width), lambda i: (0, i, 0)),
        ],
        out_specs=pl.BlockSpec((CORES, own, rows, width), lambda i: (0, 0, i, 0)),
        out_shape=jax.ShapeDtypeStruct((CORES, own, count, width), jnp.float32),
        compiler_params=pltpu.CompilerParams(vmem_limit_bytes=VMEM_LIMIT),
        name="source_window",
    )(onset_pairs, inverse, forward_table, spectrum)


def receiver_window_kernel(onset_ref, inverse_ref, forward_ref, x_ref, o_ref, buf, give, sb, ss, qs):
    p = Place()
    steps, rows, nf, _ = give.shape
    count = steps * rows
    other = (p.x * CORES + 1 - p.c, p.rec)
    barrier = pltpu.get_barrier_semaphore()
    pl.semaphore_signal(barrier, inc=1, device_id=other, device_id_type=MESH)

    def block(i):
        slot = i % 2
        src = x_ref.at[:, pl.ds(i * rows, rows)]
        return pltpu.make_async_copy(src, buf.at[slot], sb.at[slot])

    def give_copy(i):
        dst = o_ref.at[pl.ds(p.c * count + i * rows, rows)]
        return remote(give.at[i], dst, ss.at[i], qs.at[i], other)

    block(0).start()
    pl.semaphore_wait(barrier, 1)

    def step(i):
        @pl.when(i + 1 < steps)
        def _():
            block(i + 1).start()

        block(i).wait()
        inverse, forward_table = inverse_ref[...], forward_ref[p.x]
        onsets = onset_ref.at[p.c * steps + i]
        base = p.c * count + i * rows

        def store(n, value):
            o_ref[base + n] = jnp.where(p.c == 0, value[:nf], value[nf:])
            give[i, n] = jnp.where(p.c == 0, value[nf:], value[:nf])

        for start, size in groups(rows):
            window_rows(inverse, forward_table, onsets, buf.at[i % 2], start, size, store)
        give_copy(i).start()

    loop(steps, step)

    def settle(i):
        give_copy(i).wait()

    loop(steps, settle)


def receiver_window(spectrum, onset_pairs, inverse, forward_table):
    freqs, count, width = spectrum.shape
    nf = forward_table.shape[1] // 4 // CORES
    rows = rows_per_step(count)
    steps = count // rows
    onset_pairs = onset_pairs.reshape(CORES * steps, rows // 2, width)
    dma = pltpu.SemaphoreType.DMA
    return pl.pallas_call(
        receiver_window_kernel,
        in_specs=[*[IN_VMEM] * 3, ANY],
        out_specs=IN_VMEM,
        out_shape=jax.ShapeDtypeStruct((CORES * count, nf, width), jnp.float32),
        scratch_shapes=[
            pltpu.VMEM((2, freqs, rows, width), jnp.float32),
            pltpu.VMEM((steps, rows, nf, width), jnp.float32),
            dma((2,)),
            dma((steps,)),
            dma((steps,)),
        ],
        compiler_params=pltpu.CompilerParams(
            collective_id=0, has_side_effects=True, vmem_limit_bytes=VMEM_LIMIT
        ),
        name="receiver_window",
    )(onset_pairs, inverse, forward_table, spectrum)


def on_device(response_real, response_imaginary, focus, initial, onset):
    p = Place()
    nf, nr, _ = response_real.shape
    width = focus.shape[2]
    onset_pairs = onset.reshape(nr // 2, width)
    inverse, forward_table = tables(p.FQ * nf, p.X)
    spectrum, own_onset = adjoint(focus, onset_pairs, response_real, response_imaginary)
    windowed = source_window(spectrum, own_onset, inverse, forward_table)
    received = forward(windowed, response_real, response_imaginary)
    return initial - receiver_window(received, onset_pairs, inverse, forward_table)


def solution(mesh):
    return jax.shard_map(
        on_device,
        mesh=mesh,
        in_specs=(
            P("freq", "rec", None),
            P("freq", "rec", None),
            P("rec", "freq", None),
            P("rec", "freq", None),
            P("rec", None),
        ),
        out_specs=P("rec", "freq", None),
        check_vma=False,
    )
```
